32 devices in a mesh: row: 4 (over x, core), col: 8 (over z, y).
Axes of the slice: x: 2, y: 2, z: 4, core: 2. Of those that a mesh axis runs over, the one named last changes fastest.
Arguments:
- panel_rows: float32 [4096, 4096], P('row', 'col'), may hold values from -0.75 to 0.75
- owner_slot: int32 [8, 8], replicated, may hold values from -1 to 15, as said below
Outputs:
- packed: float32 [4, 16, 512, 512], P('row', 'col')
The draws below stay inside these ranges and needn't reach their ends.
Inputs may be any that keep to these rules, and one draw needn't show every extreme that they name: For j <= i, owner_slot[i, j] is the position of tile (i, j) among the 16 positions of group i // 2; tiles of one group have distinct positions; entries above the diagonal are -1. Position p lies on the device of col index p // 2.
All inputs are finite; a program needn't handle non-finite values.
Results may differ from the reference program's by a relative error of at most 0.0003.
Values sent between devices are 32-bit elements; how exact they have to be, the bound alone decides.
No kernel may reach another device: no remote copies, remote signals or barrier semaphores. Data moves between devices by JAX's collectives and lax.ppermute only.
A program may use at most 128 MiB of HBM per device.

```python
import jax
import jax.numpy as jnp
from jax import lax

BLOCK = 512
K = 4096
ORDER = 4096
BR = 2
NB = 8
POS = 16
N_ROW = 4


def draw_owner_slot(key, part):
    groups = NB // BR
    block_row = jnp.arange(NB, dtype=jnp.int32)[:, None]
    block_col = jnp.arange(NB, dtype=jnp.int32)[None, :]
    row_keys = jax.random.split(jax.random.fold_in(key, 11), groups)
    orders = jax.vmap(lambda sub_key: jax.random.permutation(sub_key, POS))(row_keys).astype(jnp.int32)
    group_ids = jnp.arange(groups, dtype=jnp.int32)
    first_rows = group_ids * BR
    tile_total = BR * first_rows + BR * (BR + 1) // 2
    picked = jax.random.randint(jax.random.fold_in(key, 12), (groups,), 0, tile_total).astype(jnp.int32)
    top_place = jnp.argmax(orders == POS - 1, axis=1).astype(jnp.int32)
    offsets = top_place - picked
    row_group = block_row // BR
    first_own = row_group * BR
    index_in = (block_row * (block_row + 1) - first_own * (first_own + 1)) // 2 + block_col
    taken = (index_in + offsets[row_group[:, 0]][:, None]) % POS
    order_rows = orders[row_group[:, 0]]
    placed = jnp.take_along_axis(order_rows, taken, axis=1)
    return jnp.where(block_col <= block_row, placed, -1).astype(jnp.int32)


def levels(stream_key, extent, cuts, low, largest):
    level, own = 1.0, jax.random.fold_in(stream_key, 6)
    for dim, parts in cuts:
        draws = jnp.exp(jax.random.uniform(jax.random.fold_in(own, dim), (parts,), jnp.float32, low / len(cuts), largest / len(cuts)))
        level = level * jnp.repeat(draws, extent[dim] // parts).reshape([-1 if axis == dim else 1 for axis in range(len(extent))])
    return level


def noise(own_key, extent, width, bound, cuts=(), held_as=jnp.bfloat16):
    result = width * jax.random.normal(own_key, extent, jnp.float32)
    if cuts:
        result = result * levels(own_key, extent, cuts, -0.22, 0.18)
    return jnp.clip(result, -bound, bound).astype(held_as)


def setup_inputs(seed: int = 0) -> dict:
    key_list = jax.random.split(jax.random.key(seed), 3)
    return {
        "panel_rows": noise(key_list[0], (ORDER, K), (K ** -0.25), 0.75, ((0, 4), (1, 8)), jnp.float32),
        "owner_slot": draw_owner_slot(jax.random.fold_in(key_list[2], 71), 0),
    }


def slot_table(owner_slot, group_id, positions, per_group):
    blocks = owner_slot.shape[0]
    block_row = jnp.arange(blocks, dtype=jnp.int32)[:, None]
    block_col = jnp.arange(blocks, dtype=jnp.int32)[None, :]
    inside = (block_row // per_group == group_id) & (block_col <= block_row)
    wanted = jnp.arange(positions, dtype=jnp.int32)[:, None, None]
    matched = inside[None] & (owner_slot[None] == wanted)
    is_live = jnp.any(matched, axis=(1, 2))
    left_block = jnp.sum(jnp.where(matched, block_row[None], 0), axis=(1, 2)).astype(jnp.int32)
    right_block = jnp.sum(jnp.where(matched, block_col[None], 0), axis=(1, 2)).astype(jnp.int32)
    return left_block, right_block, is_live


def reference(panel_rows, owner_slot):
    tiles_all = panel_rows.reshape(NB, BLOCK, K)

    def group_tiles(group_id):
        left_block, right_block, is_live = slot_table(owner_slot, group_id, POS, BR)

        def single(packed_item):
            left_one, right_one, flag = packed_item

            def compute():
                return lax.dot_general(tiles_all[left_one], tiles_all[right_one], (((1,), (1,)), ((), ())),
                                       precision=lax.Precision.HIGHEST, preferred_element_type=jnp.float32)

            def blank():
                return jnp.zeros((BLOCK, BLOCK), jnp.float32)

            return lax.cond(flag, compute, blank)

        return lax.map(single, (left_block, right_block, is_live))

    return lax.map(group_tiles, jnp.arange(N_ROW, dtype=jnp.int32))
```

```python
import functools

import jax
import jax.numpy as jnp
from jax import lax
from jax.experimental import pallas as pl
from jax.experimental.pallas import tpu as pltpu
from jax.sharding import Mesh, PartitionSpec as P

BLOCK = 512
WIDE = 256


def split_hi_lo(x):
    hi = x.astype(jnp.bfloat16)
    lo = (x - hi.astype(jnp.float32)).astype(jnp.bfloat16)
    return hi, lo


def product_kernel(dims, outs, meta_ref, pairs_ref, index_ref, s_ref, *refs):
    blocks, h, kc, ys, rb, cb, n_pairs = dims
    pieces, lists, (s_cat, j_cat, part) = refs[:4], refs[4 : 4 + outs], refs[4 + outs :]
    core = meta_ref[0]
    q = h // 2

    def put(target, row, y, x, right):
        hi, lo = split_hi_lo(x)
        base = 3 * kc * y
        rows = pl.ds(pl.multiple_of(row, q), x.shape[0])
        target[rows, base : base + kc] = hi
        target[rows, base + kc : base + 2 * kc] = lo if right else hi
        target[rows, base + 2 * kc : base + 3 * kc] = hi if right else lo

    @pl.loop(0, blocks)
    def _(j):
        for y in range(ys):
            put(s_cat, j * h, y, s_ref[y, j], False)
            for at, piece in enumerate(pieces):
                side = core if at % 2 == 0 else 1 - core
                put(j_cat, j * 2 * h + (at // 2 * 2 + side) * q, y, piece[y, j], True)

    @pl.loop(0, n_pairs)
    def _(t):
        ib, jb = pairs_ref[2 * t], pairs_ref[2 * t + 1]
        left = s_cat[pl.ds(pl.multiple_of(ib * rb, rb), rb), :]
        right = j_cat[pl.ds(pl.multiple_of(jb * cb, cb), cb), :]
        out = lax.dot_general(left, right, (((1,), (1,)), ((), ())), preferred_element_type=jnp.float32)
        for a in range(rb // h):
            for b in range(cb // (2 * h)):
                where = (ib * (rb // h) + a) * blocks + jb * (cb // (2 * h)) + b
                part[where] = out[a * h : (a + 1) * h, b * 2 * h : (b + 1) * 2 * h]

    @pl.loop(0, lists[0].shape[0])
    def _(k):
        for at, one in enumerate(lists):
            one[k] = part[index_ref[at * one.shape[0] + k]]


def products(dims, outs, n, meta, pairs, index, s, pieces):
    blocks, h, kc, ys, rb, cb, n_pairs = dims
    k3 = 3 * kc * ys
    smem, vmem = pl.BlockSpec(memory_space=pltpu.SMEM), pl.BlockSpec(memory_space=pltpu.VMEM)
    flops = 2 * n_pairs * rb * cb * k3
    return pl.pallas_call(
        functools.partial(product_kernel, dims, outs),
        out_shape=[jax.ShapeDtypeStruct((n, h, 2 * h), jnp.float32)] * outs,
        in_specs=[smem] * 3 + [vmem] * 5,
        out_specs=[vmem] * outs,
        scratch_shapes=[
            pltpu.VMEM((blocks * h, k3), jnp.bfloat16),
            pltpu.VMEM((blocks * 2 * h, k3), jnp.bfloat16),
            pltpu.VMEM((blocks * blocks, h, 2 * h), jnp.float32),
        ],
        cost_estimate=pl.CostEstimate(flops=flops, bytes_accessed=8 * s.size * 4, transcendentals=0),
    )(meta, pairs, index, s, *pieces)


def relay_kernel(up_ref, up_list_ref, down_ref, down_list_ref, up_out, down_out):
    up_out[...] = up_ref[...] + up_list_ref[...]
    down_out[...] = down_ref[...] + down_list_ref[...]


def relay(up, up_list, down, down_list):
    vmem = pl.BlockSpec(memory_space=pltpu.VMEM)
    return pl.pallas_call(
        relay_kernel,
        out_shape=[jax.ShapeDtypeStruct(up.shape, jnp.float32)] * 2,
        in_specs=[vmem] * 4,
        out_specs=[vmem] * 2,
        cost_estimate=pl.CostEstimate(flops=2 * up.size, bytes_accessed=24 * up.size, transcendentals=0),
    )(up, up_list, down, down_list)


def pick_kernel(spread_ref, live_ref, *refs):
    out_ref = refs[-1]
    devices, chunks, slots = out_ref.shape[:3]

    @pl.loop(0, devices)
    def _(d):
        for slot in range(slots):
            k = spread_ref[d * slots + slot]
            used = live_ref[d * slots + slot] > 0
            for c in range(chunks):
                total = refs[3 * c][k] + refs[3 * c + 1][k] + refs[3 * c + 2][k]
                out_ref[d, c, slot] = jnp.where(used, total, jnp.zeros_like(total))


def pick(plane, slots, spread, live, terms):
    smem, vmem = pl.BlockSpec(memory_space=pltpu.SMEM), pl.BlockSpec(memory_space=pltpu.VMEM)
    shape = (plane, len(terms) // 3, slots) + terms[0].shape[1:]
    return pl.pallas_call(
        pick_kernel,
        out_shape=jax.ShapeDtypeStruct(shape, jnp.float32),
        in_specs=[smem] * 2 + [vmem] * len(terms),
        out_specs=vmem,
    )(spread, live, *terms)


def place_kernel(plan, in_ref, out_ref):
    h, w = in_ref.shape[3:]
    q = h // 2
    for source, chip, side, parts in plan:
        for col, (first, second) in parts:
            cols = slice(col * w, (col + 1) * w)
            for half in range(2):
                row = chip * w + half * h + side * q
                rows = slice(half * q, (half + 1) * q)
                if first[0] == second[0]:
                    out_ref[:, row : row + q, cols] = in_ref[source, first[0], :, rows, :]
                else:
                    left = in_ref[source, first[0], :, rows, first[1] * h : (first[1] + 1) * h]
                    right = in_ref[source, second[0], :, rows, second[1] * h : (second[1] + 1) * h]
                    out_ref[:, row : row + q, cols] = jnp.concatenate([left, right], axis=2)


def place(plan, arrived):
    vmem = pl.BlockSpec(memory_space=pltpu.VMEM)
    return pl.pallas_call(
        functools.partial(place_kernel, plan),
        out_shape=jax.ShapeDtypeStruct((arrived.shape[2], BLOCK, BLOCK), jnp.float32),
        in_specs=[vmem],
        out_specs=vmem,
    )(arrived)


def list_tables(owner_slot, rows_n, zs, ys, slots, per_group):
    blocks = owner_slot.shape[0]
    positions = zs * ys * slots
    block_row = jnp.arange(blocks, dtype=jnp.int32)[:, None]
    block_col = jnp.arange(blocks, dtype=jnp.int32)[None, :]
    inside = block_col <= block_row
    wanted = jnp.arange(positions, dtype=jnp.int32)
    matched = (inside[None] & (owner_slot[None] == wanted[:, None, None])).reshape(positions, rows_n, per_group, blocks)
    tile_id = (block_row * blocks + block_col).reshape(1, rows_n, per_group, blocks)
    tile = jnp.sum(jnp.where(matched, tile_id, 0), axis=(2, 3))
    live = jnp.sum(matched.astype(jnp.int32), axis=(2, 3))
    entries = ys * rows_n * slots

    def by_plane(x):
        return x.reshape(zs, ys, slots, rows_n).transpose(0, 1, 3, 2).reshape(zs, entries)

    tile, live = by_plane(tile), by_plane(live)
    order = jnp.arange(entries, dtype=jnp.int32)
    before = order[None, :, None] > order[None, None, :]
    rank = jnp.sum(jnp.where(before, live[:, None, :], 0), axis=2)
    hit = (rank[:, None, :] == order[None, :, None]) & (live[:, None, :] > 0)
    index = jnp.sum(jnp.where(hit, tile[:, None, :], 0), axis=2)
    longest = jnp.max(jnp.sum(live, axis=1))
    return index, rank, live, longest


def make_plan(chips, zs):
    singles = [u for u in range(1, chips) if u & (u - 1) == 0]
    chunks = [((0, 0), (0, 1))]
    if len(singles) > 1:
        chunks += [((singles[-1], half), (singles[0], half)) for half in range(2)]
    used = {u for chunk in chunks for u, _ in chunk}
    chunks += [((u, 0), (u, 1)) for u in range(1, chips) if u not in used]
    events = []
    for c in range(len(chunks)):
        events.append((3 * c, "product", c, 0))
        events.extend((3 * c + 2.2 * (step - 1), "step", c, step) for step in range(2, zs))
        if c:
            events.append((3 * c - 1.5, "fetch", c, 0))
    events.sort(key=lambda e: e[0])
    return chunks, events


def link_of(u, half):
    return u & -u if half == 0 else 1 << (u.bit_length() - 1)


def body(panel_rows, owner_slot):
    rows_n, zs, ys = (lax.axis_size(name) for name in ("row", "z", "y"))
    slab_rows, kc = panel_rows.shape
    per_group = slab_rows // BLOCK
    blocks = per_group * rows_n
    cols_n = zs * ys
    row_tiles = per_group * (blocks - per_group) + per_group * (per_group + 1) // 2
    slots = (row_tiles + cols_n - 1) // cols_n
    plane = rows_n * ys
    chips = plane // 2
    h = BLOCK // plane
    rb, cb = min(WIDE, blocks * h), min(WIDE, blocks * 2 * h)
    per_i, per_j = rb // h, cb // (2 * h)
    pair_list = [
        (ib, jb)
        for ib in range(blocks // per_i)
        for jb in range(blocks // per_j)
        if ib * per_i + per_i - 1 >= jb * per_j
    ]
    dims = (blocks, h, kc, ys, rb, cb, len(pair_list))
    pairs = jnp.array([v for pair in pair_list for v in pair], jnp.int32)
    my_z, my_row, my_y = (lax.axis_index(name) for name in ("z", "row", "y"))
    meta = jnp.stack([my_row % 2, (my_row // 2) * ys + my_y]).astype(jnp.int32)
    index, rank, live, longest = list_tables(owner_slot, rows_n, zs, ys, slots, per_group)
    entries = ys * rows_n * slots

    steps = range(1, zs)
    wanted = [my_z + zs - step for step in steps] + [my_z - zs + step for step in steps] + [my_z]
    wanted = jnp.clip(jnp.stack(wanted), 0, zs - 1)
    at_plane = (wanted[:, None] == jnp.arange(zs)[None, :])[:, :, None]
    index = jnp.sum(jnp.where(at_plane, index[None], 0), axis=1)
    own = (jnp.arange(zs) == my_z)[:, None]
    my_rank, my_live = (jnp.sum(jnp.where(own, table, 0), axis=0) for table in (rank, live))

    def chip_swap(x, u):
        ux, uy = u // ys, u % ys
        if uy == 0:
            return lax.ppermute(x, "row", [(r, r ^ (2 * ux)) for r in range(rows_n)])
        if ux == 0:
            return lax.ppermute(x, "y", [(y, y ^ uy) for y in range(ys)])
        perm = [(r * ys + y, (r ^ (2 * ux)) * ys + (y ^ uy)) for r in range(rows_n) for y in range(ys)]
        return lax.ppermute(x, ("row", "y"), perm)

    def core_swap(x):
        return lax.ppermute(x, "row", [(r, r ^ 1) for r in range(rows_n)])

    chunks, events = make_plan(chips, zs)

    def run(n, *args):
        return run_scoped(n, *args)

    def run_scoped(n, panel, index, my_rank, my_live):
        sliced = panel.reshape(per_group, rows_n // 2, ys, 2, 2, h // 2, kc).transpose(2, 1, 4, 0, 3, 5, 6)
        sliced = sliced.reshape(plane, per_group, h, kc)
        s = lax.all_to_all(sliced, ("y", "row"), 0, 0, tiled=True).reshape(ys, blocks, h, kc)
        same, peer = {(0, 0): s[:, :, : h // 2], (0, 1): s[:, :, h // 2 :]}, {}

        def cores(u, half):
            peer[u, half] = core_swap(same[u, half])

        def reach(u, half):
            if (u, half) not in same:
                low = link_of(u, half)
                reach(u ^ low, half)
                same[u, half] = chip_swap(same[u ^ low, half], low)

        for half in range(2):
            cores(0, half)
            for u in range(1, chips):
                reach(u, half)
        flat_index = index[:, :n].reshape(-1)
        lists, flows = {}, {}

        def forward(c, step, up, down):
            up = lax.ppermute(up, "z", [(z, z + 1) for z in range(step)])
            down = lax.ppermute(down, "z", [(zs - 1 - z, zs - 2 - z) for z in range(step)])
            flows[c] = (up, down)

        for _, kind, c, step in events:
            if kind == "fetch":
                for u, half in chunks[c]:
                    cores(u, half)
            elif kind == "product":
                pieces = [side[key] for key in chunks[c] for side in (same, peer)]
                lists[c] = products(dims, 2 * zs - 1, n, meta, pairs, flat_index, s, pieces)
                forward(c, 1, lists[c][0], lists[c][zs - 1])
            else:
                up, down = relay(flows[c][0], lists[c][step - 1], flows[c][1], lists[c][zs + step - 2])
                forward(c, step, up, down)

        terms = [x for c in range(len(chunks)) for x in (lists[c][-1], *flows[c])]
        ready = pick(plane, slots, jnp.minimum(my_rank, n - 1), my_live, terms)
        arrived = lax.all_to_all(ready, ("y", "row"), 0, 0, tiled=True)
        plan = []
        for d in range(plane):
            chip = (d % rows_n) // 2 * ys + d // rows_n
            parts = []
            for u in range(chips):
                spots = []
                for half in range(2):
                    c = next(i for i, chunk in enumerate(chunks) if (u, half) in chunk)
                    spots.append((c, chunks[c].index((u, half))))
                parts.append((chip ^ u, tuple(spots)))
            plan.append((d, chip, d % 2, tuple(parts)))
        return place(tuple(plan), arrived)[None]

    mean = (blocks * (blocks + 1) // 2 + zs - 1) // zs
    sizes = sorted({min(entries, mean + extra) for extra in (3,)} | {entries})
    which = sum((longest > size).astype(jnp.int32) for size in sizes[:-1])
    branches = [functools.partial(run, size) for size in sizes]
    return lax.switch(which, branches, panel_rows, index, my_rank, my_live)


def solution(mesh):
    rows_n, cols_n = mesh.shape["row"], mesh.shape["col"]
    ys = 2 if cols_n % 2 == 0 else 1
    fine = Mesh(mesh.devices.reshape(rows_n, cols_n // ys, ys), ("row", "z", "y"))
    return jax.shard_map(
        body,
        mesh=fine,
        in_specs=(P("row", ("z", "y")), P()),
        out_specs=P("row", ("z", "y"), None, None),
        check_vma=False,
    )
```

```python
import functools

import jax
import jax.numpy as jnp
from jax import lax
from jax.experimental import pallas as pl
from jax.experimental.pallas import tpu as pltpu
from jax.sharding import Mesh, PartitionSpec as P

BLOCK = 512
WIDE = 256


def split_hi_lo(x):
    hi = x.astype(jnp.bfloat16)
    lo = (x - hi.astype(jnp.float32)).astype(jnp.bfloat16)
    return hi, lo


def product_kernel(dims, outs, meta_ref, pairs_ref, index_ref, s_ref, *refs):
    blocks, h, kc, ys, rb, cb, n_pairs = dims
    pieces, lists, (s_cat, j_cat, part) = refs[:4], refs[4 : 4 + outs], refs[4 + outs :]
    core = meta_ref[0]
    q = h // 2

    def put(target, row, y, x, right):
        hi, lo = split_hi_lo(x)
        base = 3 * kc * y
        rows = pl.ds(pl.multiple_of(row, q), x.shape[0])
        target[rows, base : base + kc] = hi
        target[rows, base + kc : base + 2 * kc] = lo if right else hi
        target[rows, base + 2 * kc : base + 3 * kc] = hi if right else lo

    @pl.loop(0, blocks)
    def _(j):
        for y in range(ys):
            put(s_cat, j * h, y, s_ref[y, j], False)
            for at, piece in enumerate(pieces):
                side = core if at % 2 == 0 else 1 - core
                put(j_cat, j * 2 * h + (at // 2 * 2 + side) * q, y, piece[y, j], True)

    @pl.loop(0, n_pairs)
    def _(t):
        ib, jb = pairs_ref[2 * t], pairs_ref[2 * t + 1]
        left = s_cat[pl.ds(pl.multiple_of(ib * rb, rb), rb), :]
        right = j_cat[pl.ds(pl.multiple_of(jb * cb, cb), cb), :]
        out = lax.dot_general(left, right, (((1,), (1,)), ((), ())), preferred_element_type=jnp.float32)
        for a in range(rb // h):
            for b in range(cb // (2 * h)):
                where = (ib * (rb // h) + a) * blocks + jb * (cb // (2 * h)) + b
                part[where] = out[a * h : (a + 1) * h, b * 2 * h : (b + 1) * 2 * h]

    base = 0
    for one in lists:

        @pl.loop(0, one.shape[0])
        def _(k, one=one, base=base):
            one[k] = part[index_ref[base + k]]

        base += one.shape[0]


def products(dims, sizes, meta, pairs, index, s, pieces):
    blocks, h, kc, ys, rb, cb, n_pairs = dims
    outs = len(sizes)
    k3 = 3 * kc * ys
    smem, vmem = pl.BlockSpec(memory_space=pltpu.SMEM), pl.BlockSpec(memory_space=pltpu.VMEM)
    flops = 2 * n_pairs * rb * cb * k3
    return pl.pallas_call(
        functools.partial(product_kernel, dims, outs),
        out_shape=[jax.ShapeDtypeStruct((size, h, 2 * h), jnp.float32) for size in sizes],
        in_specs=[smem] * 3 + [vmem] * 5,
        out_specs=[vmem] * outs,
        scratch_shapes=[
            pltpu.VMEM((blocks * h, k3), jnp.bfloat16),
            pltpu.VMEM((blocks * 2 * h, k3), jnp.bfloat16),
            pltpu.VMEM((blocks * blocks, h, 2 * h), jnp.float32),
        ],
        cost_estimate=pl.CostEstimate(flops=flops, bytes_accessed=8 * s.size * 4, transcendentals=0),
    )(meta, pairs, index, s, *pieces)


def pick_kernel(chunks, spread_ref, live_ref, *refs):
    out_ref = refs[-1]
    devices, _, slots = out_ref.shape[:3]
    entries = devices * slots
    each = (len(refs) - 1) // chunks

    @pl.loop(0, devices)
    def _(d):
        for slot in range(slots):
            e = d * slots + slot
            used = live_ref[e] > 0
            for c in range(chunks):
                total = refs[each * c][e]
                for step in range(1, each):
                    total += refs[each * c + step][spread_ref[(step - 1) * entries + e]]
                out_ref[d, c, slot] = jnp.where(used, total, jnp.zeros_like(total))


def pick(plane, slots, chunks, spread, live, terms):
    smem, vmem = pl.BlockSpec(memory_space=pltpu.SMEM), pl.BlockSpec(memory_space=pltpu.VMEM)
    shape = (plane, chunks, slots) + terms[0].shape[1:]
    return pl.pallas_call(
        functools.partial(pick_kernel, chunks),
        out_shape=jax.ShapeDtypeStruct(shape, jnp.float32),
        in_specs=[smem] * 2 + [vmem] * len(terms),
        out_specs=vmem,
    )(spread, live, *terms)


def place_kernel(plan, *refs):
    in_refs, out_ref = refs[:-1], refs[-1]
    h, w = in_refs[0].shape[3:]
    q = h // 2
    for source, chip, side, parts in plan:
        for col, spots in parts:
            cols = slice(col * w, (col + 1) * w)
            first, second = spots[0][0], spots[1][0]
            for half in range(2):
                row = chip * w + half * h + side * q
                rows = slice(half * q, (half + 1) * q)
                if first == second:
                    out_ref[:, row : row + q, cols] = in_refs[first[0]][source, first[1], :, rows, :]
                else:
                    halves = []
                    for (group, at), spot in spots:
                        halves.append(in_refs[group][source, at, :, rows, spot * h : (spot + 1) * h])
                    out_ref[:, row : row + q, cols] = jnp.concatenate(halves, axis=2)


def place(plan, arrived):
    vmem = pl.BlockSpec(memory_space=pltpu.VMEM)
    return pl.pallas_call(
        functools.partial(place_kernel, plan),
        out_shape=jax.ShapeDtypeStruct((arrived[0].shape[2], BLOCK, BLOCK), jnp.float32),
        in_specs=[vmem] * len(arrived),
        out_specs=vmem,
    )(*arrived)


def list_tables(owner_slot, rows_n, zs, ys, slots, per_group):
    blocks = owner_slot.shape[0]
    positions = zs * ys * slots
    block_row = jnp.arange(blocks, dtype=jnp.int32)[:, None]
    block_col = jnp.arange(blocks, dtype=jnp.int32)[None, :]
    inside = block_col <= block_row
    wanted = jnp.arange(positions, dtype=jnp.int32)
    matched = (inside[None] & (owner_slot[None] == wanted[:, None, None])).reshape(positions, rows_n, per_group, blocks)
    tile_id = (block_row * blocks + block_col).reshape(1, rows_n, per_group, blocks)
    tile = jnp.sum(jnp.where(matched, tile_id, 0), axis=(2, 3))
    live = jnp.sum(matched.astype(jnp.int32), axis=(2, 3))
    entries = ys * rows_n * slots

    def by_plane(x):
        return x.reshape(zs, ys, slots, rows_n).transpose(0, 1, 3, 2).reshape(zs, entries)

    tile, live = by_plane(tile), by_plane(live)
    order = jnp.arange(entries, dtype=jnp.int32)
    before = order[None, :, None] > order[None, None, :]
    rank = jnp.sum(jnp.where(before, live[:, None, :], 0), axis=2)
    count = jnp.sum(live, axis=1)
    return tile, live, rank, count


def make_plan(chips, zs):
    singles = [u for u in range(1, chips) if u & (u - 1) == 0]
    chunks = [((0, 0), (0, 1))]
    if len(singles) > 1:
        chunks += [((singles[-1], half), (singles[0], half)) for half in range(2)]
    used = {u for chunk in chunks for u, _ in chunk}
    chunks += [((u, 0), (u, 1)) for u in range(1, chips) if u not in used]
    gap = 2 if len(chunks) <= 4 else 2 * zs
    events = []
    for c in range(len(chunks)):
        events.append((gap * c, "product", c, 0))
        events.extend((gap * c + 2 * step - 1.8 + 0.01 * step, "step", c, step) for step in range(2, zs))
        if c:
            events.append((gap * c - 0.5, "fetch", c, 0))
    groups = [list(range(c, min(c + 2, len(chunks)))) for c in range(0, len(chunks), 2)]
    events.extend((gap * group[-1] + 2 * zs - 1.7, "early", at, 0) for at, group in enumerate(groups[:-1]))
    events.sort(key=lambda e: e[0])
    return chunks, events, groups


def link_of(u, half):
    return u & -u if half == 0 else 1 << (u.bit_length() - 1)


def body(panel_rows, owner_slot):
    rows_n, zs, ys = (lax.axis_size(name) for name in ("row", "z", "y"))
    slab_rows, kc = panel_rows.shape
    per_group = slab_rows // BLOCK
    blocks = per_group * rows_n
    cols_n = zs * ys
    row_tiles = per_group * (blocks - per_group) + per_group * (per_group + 1) // 2
    slots = (row_tiles + cols_n - 1) // cols_n
    plane = rows_n * ys
    chips = plane // 2
    h = BLOCK // plane
    rb, cb = min(WIDE, blocks * h), min(2 * WIDE, blocks * 2 * h)
    per_i, per_j = rb // h, cb // (2 * h)
    pair_list = [
        (ib, jb)
        for ib in range(blocks // per_i)
        for jb in range(blocks // per_j)
        if ib * per_i + per_i - 1 >= jb * per_j
    ]
    dims = (blocks, h, kc, ys, rb, cb, len(pair_list))
    pairs = jnp.array([v for pair in pair_list for v in pair], jnp.int32)
    my_z, my_row, my_y = (lax.axis_index(name) for name in ("z", "row", "y"))
    meta = jnp.stack([my_row % 2, (my_row // 2) * ys + my_y]).astype(jnp.int32)
    sliced = panel_rows.reshape(per_group, rows_n // 2, ys, 2, 2, h // 2, kc).transpose(2, 1, 4, 0, 3, 5, 6)
    sliced = sliced.reshape(plane, per_group, h, kc)
    s = lax.all_to_all(sliced, ("y", "row"), 0, 0, tiled=True).reshape(ys, blocks, h, kc)
    tile, live, rank, count = list_tables(owner_slot, rows_n, zs, ys, slots, per_group)
    entries = ys * rows_n * slots
    tiles = blocks * (blocks + 1) // 2

    planes = jnp.arange(zs, dtype=jnp.int32)
    above = jnp.sum(jnp.where(planes[None, :] > planes[:, None], count[None, :], 0), axis=1)
    below = jnp.sum(jnp.where(planes[None, :] < planes[:, None], count[None, :], 0), axis=1)
    up_at, down_at = above[:, None] + rank, below[:, None] + rank
    places = jnp.arange(tiles, dtype=jnp.int32)

    def in_order(at):
        hit = (at[None] == places[:, None, None]) & (live[None] > 0)
        return jnp.sum(jnp.where(hit, tile[None], 0), axis=(1, 2))

    up_order, down_order = in_order(up_at), in_order(down_at)
    own = (planes == my_z)[:, None]
    my_tile, my_live, my_up, my_down = (jnp.sum(jnp.where(own, t, 0), axis=0) for t in (tile, live, up_at, down_at))
    index = jnp.stack([jnp.where(my_z == step - 1, up_order, down_order) for step in range(1, zs)])
    spread = jnp.stack(
        [jnp.where(my_z == step, my_up, jnp.where(my_z == zs - 1 - step, my_down, 0)) for step in range(1, zs)]
    )
    needed = [jnp.maximum(above[step - 1], below[zs - step]) for step in range(1, zs)]

    def chip_swap(x, u):
        ux, uy = u // ys, u % ys
        if uy == 0:
            return lax.ppermute(x, "row", [(r, r ^ (2 * ux)) for r in range(rows_n)])
        if ux == 0:
            return lax.ppermute(x, "y", [(y, y ^ uy) for y in range(ys)])
        perm = [(r * ys + y, (r ^ (2 * ux)) * ys + (y ^ uy)) for r in range(rows_n) for y in range(ys)]
        return lax.ppermute(x, ("row", "y"), perm)

    def core_swap(x):
        return lax.ppermute(x, "row", [(r, r ^ 1) for r in range(rows_n)])

    chunks, events, groups = make_plan(chips, zs)

    def run(sizes, *args):
        return run_scoped(sizes, *args)

    def run_scoped(sizes, s, index, spread, my_tile, my_live):
        same, peer = {(0, 0): s[:, :, : h // 2], (0, 1): s[:, :, h // 2 :]}, {}

        def cores(u, half):
            peer[u, half] = core_swap(same[u, half])

        def reach(u, half):
            if (u, half) not in same:
                low = link_of(u, half)
                reach(u ^ low, half)
                same[u, half] = chip_swap(same[u ^ low, half], low)

        for half in range(2):
            cores(0, half)
            for u in range(1, chips):
                reach(u, half)
        flat_index = jnp.concatenate([index[i, :size] for i, size in enumerate(sizes)] + [my_tile])
        limit = jnp.array(sizes, jnp.int32)[:, None] - 1
        flat_spread = jnp.minimum(spread, limit).reshape(-1)
        lists, flows, arrived = {}, {}, []

        def forward(c, step, x):
            flows[c, step] = lax.ppermute(x, "z", [(step - 1, step), (zs - step, zs - step - 1)])

        def deliver(group):
            terms = [x for c in group for x in (lists[c][-1], *(flows[c, step] for step in range(1, zs)))]
            ready = pick(plane, slots, len(group), flat_spread, my_live, terms)
            arrived.append(lax.all_to_all(ready, ("y", "row"), 0, 0, tiled=True))

        for _, kind, c, step in events:
            if kind == "fetch":
                for u, half in chunks[c]:
                    cores(u, half)
            elif kind == "product":
                pieces = [side[key] for key in chunks[c] for side in (same, peer)]
                lists[c] = products(dims, (*sizes, entries), meta, pairs, flat_index, s, pieces)
                forward(c, 1, lists[c][0])
            elif kind == "step":
                own = lists[c][step - 1]
                passed = flows[c, step - 1][: own.shape[0]] + own
                forward(c, step, passed)
            else:
                deliver(groups[c])

        deliver(groups[-1])
        plan = []
        for d in range(plane):
            chip = (d % rows_n) // 2 * ys + d // rows_n
            parts = []
            for u in range(chips):
                spots = []
                for half in range(2):
                    c = next(i for i, chunk in enumerate(chunks) if (u, half) in chunk)
                    where = next((g, group.index(c)) for g, group in enumerate(groups) if c in group)
                    spots.append((where, chunks[c].index((u, half))))
                parts.append((chip ^ u, tuple(spots)))
            plan.append((d, chip, d % 2, tuple(parts)))
        return place(tuple(plan), arrived)[None]

    mean = [-(-tiles * (zs - step) // zs) for step in range(1, zs)]
    whole = tuple(min(tiles, (zs - step) * entries) for step in range(1, zs))
    sizes = [tuple(min(m + extra, w) for m, w, extra in zip(mean, whole, (low, *[low + 1] * zs))) for low in (1, 3)]
    which = 0
    for choice in sizes:
        fits = functools.reduce(jnp.logical_and, [need <= size for need, size in zip(needed, choice)])
        which += 1 - fits.astype(jnp.int32)
    sizes.append(whole)
    branches = [functools.partial(run, size) for size in sizes]
    return lax.switch(which, branches, s, index, spread, my_tile, my_live)


def solution(mesh):
    rows_n, cols_n = mesh.shape["row"], mesh.shape["col"]
    ys = 2 if cols_n % 2 == 0 else 1
    fine = Mesh(mesh.devices.reshape(rows_n, cols_n // ys, ys), ("row", "z", "y"))
    return jax.shard_map(
        body,
        mesh=fine,
        in_specs=(P("row", ("z", "y")), P()),
        out_specs=P("row", ("z", "y"), None, None),
        check_vma=False,
    )
```

```python
import functools

import jax
import jax.numpy as jnp
from jax import lax
from jax.experimental import pallas as pl
from jax.experimental.pallas import tpu as pltpu
from jax.sharding import Mesh, PartitionSpec as P

BLOCK = 512
WIDE = 256


def split_hi_lo(x):
    hi = x.astype(jnp.bfloat16)
    lo = (x - hi.astype(jnp.float32)).astype(jnp.bfloat16)
    return hi, lo


def put_parts(target, row, y, x, order):
    parts = split_hi_lo(x)
    kc = x.shape[1]
    rows = pl.ds(pl.multiple_of(row, x.shape[0]), x.shape[0])
    for at, which in enumerate(order):
        col = (3 * y + at) * kc
        target[rows, col : col + kc] = parts[which]


def put_right(core, pieces, right):
    ys, blocks, q, _ = pieces[0].shape

    @pl.loop(0, blocks)
    def _(j):
        for y in range(ys):
            for at, piece in enumerate(pieces):
                side = core if at % 2 == 0 else 1 - core
                put_parts(right, (4 * j + at // 2 * 2 + side) * q, y, piece[y, j], (0, 1, 0))


def prepare_kernel(meta_ref, *refs):
    put_right(meta_ref[0], refs[:4], refs[4])


def prepare(meta, pieces):
    ys, blocks, q, kc = pieces[0].shape
    vmem = pl.BlockSpec(memory_space=pltpu.VMEM)
    return pl.pallas_call(
        prepare_kernel,
        out_shape=jax.ShapeDtypeStruct((blocks * 4 * q, 3 * kc * ys), jnp.bfloat16),
        in_specs=[pl.BlockSpec(memory_space=pltpu.SMEM)] + [vmem] * 4,
        out_specs=vmem,
        cost_estimate=pl.CostEstimate(flops=2**28, bytes_accessed=40 * pieces[0].size, transcendentals=0),
    )(meta, *pieces)


def product_kernel(dims, outs, first, meta_ref, pairs_ref, index_ref, *refs):
    blocks, h, _, ys, rb, cb, n_pairs = dims
    n_in = 4 if first else 3
    hbm, lists, (left, part, right, sems, *held) = refs[:n_in], refs[n_in:][:outs], refs[n_in + outs :]
    q = h // 2

    def right_copy(jb):
        rows = pl.ds(pl.multiple_of(jb * cb, cb), cb)
        return pltpu.make_async_copy(hbm[2].at[rows], right.at[rows], sems.at[2 + jb])

    copies = [pltpu.make_async_copy(hbm[i], held[i], sems.at[i]) for i in range(len(held))]
    for copy in copies:
        copy.start()
    if not first:
        for jb in range(right.shape[0] // cb):
            right_copy(jb).start()
    for copy in copies[:2]:
        copy.wait()

    @pl.loop(0, blocks)
    def _(i):
        for y in range(ys):
            for slot in range(2):
                put_parts(left, i * h + slot * q, y, held[slot][y, i], (0, 0, 1))

    if first:
        for copy in copies[2:]:
            copy.wait()
        put_right(meta_ref[0], (held[0], held[2], held[1], held[3]), right)

    @pl.loop(0, n_pairs)
    def _(t):
        ib, jb = pairs_ref[3 * t], pairs_ref[3 * t + 1]
        if not first:

            @pl.when(pairs_ref[3 * t + 2] == 1)
            def _():
                right_copy(jb).wait()

        rows, cols = pl.ds(pl.multiple_of(ib * rb, rb), rb), pl.ds(pl.multiple_of(jb * cb, cb), cb)
        out = lax.dot_general(left[rows, :], right[cols, :], (((1,), (1,)), ((), ())), preferred_element_type=jnp.float32)
        for a in range(rb // h):
            for b in range(cb // (2 * h)):
                where = (ib * (rb // h) + a) * blocks + jb * (cb // (2 * h)) + b
                part[where] = out[a * h : (a + 1) * h, b * 2 * h : (b + 1) * 2 * h]

    base = 0
    for one in lists:

        @pl.loop(0, one.shape[0])
        def _(k, one=one, base=base):
            one[k] = part[index_ref[base + k]]

        base += one.shape[0]


def products(dims, sizes, meta, pairs, index, pieces, rights):
    blocks, h, kc, ys, rb, cb, n_pairs = dims
    k3 = 3 * kc * ys
    first = len(rights) == 2
    smem, vmem = pl.BlockSpec(memory_space=pltpu.SMEM), pl.BlockSpec(memory_space=pltpu.VMEM)
    flops = 2 * n_pairs * rb * cb * k3
    return pl.pallas_call(
        functools.partial(product_kernel, dims, len(sizes), first),
        out_shape=[jax.ShapeDtypeStruct((size, h, 2 * h), jnp.float32) for size in sizes],
        in_specs=[smem] * 3 + [pl.BlockSpec(memory_space=pl.ANY)] * (2 + len(rights)),
        out_specs=[vmem] * len(sizes),
        scratch_shapes=[
            pltpu.VMEM((blocks * h, k3), jnp.bfloat16),
            pltpu.VMEM((blocks * blocks, h, 2 * h), jnp.float32),
            pltpu.VMEM((blocks * 2 * h, k3), jnp.bfloat16),
            pltpu.SemaphoreType.DMA((max(4, 2 + blocks * 2 * h // cb),)),
            *[pltpu.VMEM(pieces[0].shape, jnp.float32)] * (4 if first else 2),
        ],
        cost_estimate=pl.CostEstimate(flops=flops, bytes_accessed=4 * blocks * h * k3, transcendentals=0),
    )(meta, pairs, index, *pieces, *rights)


def pick_kernel(chunks, spread_ref, live_ref, *refs):
    out_ref = refs[-1]
    devices, _, slots = out_ref.shape[:3]
    entries = devices * slots
    each = (len(refs) - 1) // chunks

    @pl.loop(0, devices)
    def _(d):
        for slot in range(slots):
            e = d * slots + slot
            used = live_ref[e] > 0
            for c in range(chunks):
                total = refs[each * c][e]
                for step in range(1, each):
                    total += refs[each * c + step][spread_ref[(step - 1) * entries + e]]
                out_ref[d, c, slot] = jnp.where(used, total, jnp.zeros_like(total))


def pick(plane, slots, chunks, spread, live, terms):
    smem, vmem = pl.BlockSpec(memory_space=pltpu.SMEM), pl.BlockSpec(memory_space=pltpu.VMEM)
    shape = (plane, chunks, slots) + terms[0].shape[1:]
    return pl.pallas_call(
        functools.partial(pick_kernel, chunks),
        out_shape=jax.ShapeDtypeStruct(shape, jnp.float32),
        in_specs=[smem] * 2 + [vmem] * len(terms),
        out_specs=vmem,
    )(spread, live, *terms)


def place_kernel(plan, *refs):
    in_refs, out_ref = refs[:-1], refs[-1]
    h, w = in_refs[0].shape[3:]
    q = h // 2
    for source, group, at, slot, row, col in plan:
        rows = slice(slot * q, (slot + 1) * q)
        out_ref[:, row : row + q, col : col + w] = in_refs[group][source, at, :, rows, :]


def place(plan, arrived):
    vmem = pl.BlockSpec(memory_space=pltpu.VMEM)
    return pl.pallas_call(
        functools.partial(place_kernel, plan),
        out_shape=jax.ShapeDtypeStruct((arrived[0].shape[2], BLOCK, BLOCK), jnp.float32),
        in_specs=[vmem] * len(arrived),
        out_specs=vmem,
    )(*arrived)


def list_tables(owner_slot, rows_n, zs, ys, slots, per_group):
    blocks = owner_slot.shape[0]
    positions = zs * ys * slots
    block_row = jnp.arange(blocks, dtype=jnp.int32)[:, None]
    block_col = jnp.arange(blocks, dtype=jnp.int32)[None, :]
    inside = block_col <= block_row
    wanted = jnp.arange(positions, dtype=jnp.int32)
    matched = (inside[None] & (owner_slot[None] == wanted[:, None, None])).reshape(positions, rows_n, per_group, blocks)
    tile_id = (block_row * blocks + block_col).reshape(1, rows_n, per_group, blocks)
    tile = jnp.sum(jnp.where(matched, tile_id, 0), axis=(2, 3))
    live = jnp.sum(matched.astype(jnp.int32), axis=(2, 3))
    entries = ys * rows_n * slots

    def by_plane(x):
        return x.reshape(zs, ys, slots, rows_n).transpose(0, 1, 3, 2).reshape(zs, entries)

    tile, live = by_plane(tile), by_plane(live)
    order = jnp.arange(entries, dtype=jnp.int32)
    before = order[None, :, None] > order[None, None, :]
    rank = jnp.sum(jnp.where(before, live[:, None, :], 0), axis=2)
    count = jnp.sum(live, axis=1)
    return tile, live, rank, count


def make_plan(chips, zs):
    singles = [u for u in range(1, chips) if u & (u - 1) == 0]
    chunks = [((0, 0), (0, 1))]
    if len(singles) > 1:
        chunks += [((singles[-1], half), (singles[0], half)) for half in range(2)]
    used = {u for chunk in chunks for u, _ in chunk}
    chunks += [((u, 0), (u, 1)) for u in range(1, chips) if u not in used]
    gap = 2 if len(chunks) <= 4 else 2 * zs
    events = []
    for c in range(len(chunks)):
        events.append((gap * c, "product", c, 0))
        events.extend((gap * c + 2 * step - 1.8 + 0.01 * step, "step", c, step) for step in range(2, zs))
    if len(chunks) > 1:
        events.append((0.1, "prepare", 0, 0))
    for u in range(1, chips):
        if u not in singles:
            events.extend((gap * (1 + half) + 0.1 - 0.2 * half, "chip", u, half) for half in range(2))
    groups = [list(range(c, min(c + 2, len(chunks)))) for c in range(0, len(chunks), 2)]
    events.extend((gap * group[-1] + 2 * zs - 1.7, "early", at, 0) for at, group in enumerate(groups[:-1]))
    events.sort(key=lambda e: e[0])
    return chunks, events, groups


def link_of(u, half):
    return u & -u if half == 0 else 1 << (u.bit_length() - 1)


def body(panel_rows, owner_slot):
    rows_n, zs, ys = (lax.axis_size(name) for name in ("row", "z", "y"))
    slab_rows, kc = panel_rows.shape
    per_group = slab_rows // BLOCK
    blocks = per_group * rows_n
    cols_n = zs * ys
    row_tiles = per_group * (blocks - per_group) + per_group * (per_group + 1) // 2
    slots = (row_tiles + cols_n - 1) // cols_n
    plane = rows_n * ys
    chips = plane // 2
    h = BLOCK // plane
    rb, cb = min(WIDE, blocks * h), min(2 * WIDE, blocks * 2 * h)
    per_i, per_j = rb // h, cb // (2 * h)
    pair_list = []
    for jb in range(blocks // per_j):
        rows = [ib for ib in range(blocks // per_i) if ib * per_i + per_i - 1 >= jb * per_j]
        pair_list += [(ib, jb, int(ib == rows[0])) for ib in rows]
    dims = (blocks, h, kc, ys, rb, cb, len(pair_list))
    pairs = jnp.array([v for pair in pair_list for v in pair], jnp.int32)
    my_z, my_row, my_y = (lax.axis_index(name) for name in ("z", "row", "y"))
    meta = jnp.stack([my_row % 2, (my_row // 2) * ys + my_y]).astype(jnp.int32)
    sliced = panel_rows.reshape(per_group, rows_n // 2, ys, 2, 2, h // 2, kc).transpose(2, 1, 4, 0, 3, 5, 6)
    sliced = sliced.reshape(plane, per_group, h, kc)
    s = lax.all_to_all(sliced, ("y", "row"), 0, 0, tiled=True).reshape(ys, blocks, h, kc)
    tile, live, rank, count = list_tables(owner_slot, rows_n, zs, ys, slots, per_group)
    entries = ys * rows_n * slots
    tiles = blocks * (blocks + 1) // 2

    planes = jnp.arange(zs, dtype=jnp.int32)
    above = jnp.sum(jnp.where(planes[None, :] > planes[:, None], count[None, :], 0), axis=1)
    below = jnp.sum(jnp.where(planes[None, :] < planes[:, None], count[None, :], 0), axis=1)
    up_at, down_at = above[:, None] + rank, below[:, None] + rank
    places = jnp.arange(tiles, dtype=jnp.int32)

    def in_order(at):
        hit = (at[None] == places[:, None, None]) & (live[None] > 0)
        return jnp.sum(jnp.where(hit, tile[None], 0), axis=(1, 2))

    up_order, down_order = in_order(up_at), in_order(down_at)
    own = (planes == my_z)[:, None]
    my_tile, my_live, my_up, my_down = (jnp.sum(jnp.where(own, t, 0), axis=0) for t in (tile, live, up_at, down_at))
    index = jnp.stack([jnp.where(my_z == step - 1, up_order, down_order) for step in range(1, zs)])
    spread = jnp.stack(
        [jnp.where(my_z == step, my_up, jnp.where(my_z == zs - 1 - step, my_down, 0)) for step in range(1, zs)]
    )
    needed = [jnp.maximum(above[step - 1], below[zs - step]) for step in range(1, zs)]

    def chip_swap(x, u):
        ux, uy = u // ys, u % ys
        if uy == 0:
            return lax.ppermute(x, "row", [(r, r ^ (2 * ux)) for r in range(rows_n)])
        if ux == 0:
            return lax.ppermute(x, "y", [(y, y ^ uy) for y in range(ys)])
        perm = [(r * ys + y, (r ^ (2 * ux)) * ys + (y ^ uy)) for r in range(rows_n) for y in range(ys)]
        return lax.ppermute(x, ("row", "y"), perm)

    def core_swap(x):
        return lax.ppermute(x, "row", [(r, r ^ 1) for r in range(rows_n)])

    chunks, events, groups = make_plan(chips, zs)

    def run(sizes, *args):
        return run_scoped(sizes, *args)

    def run_scoped(sizes, s, index, spread, my_tile, my_live):
        same, peer = {(0, 0): s[:, :, : h // 2], (0, 1): s[:, :, h // 2 :]}, {}

        def reach(u, half):
            if (u, half) not in same:
                low = link_of(u, half)
                reach(u ^ low, half)
                same[u, half] = chip_swap(same[u ^ low, half], low)

        for half in range(2):
            peer[half] = core_swap(same[0, half])
            for u in range(1, chips):
                reach(u, half)
        flat_index = jnp.concatenate([index[i, :size] for i, size in enumerate(sizes)] + [my_tile])
        limit = jnp.array(sizes, jnp.int32)[:, None] - 1
        flat_spread = jnp.minimum(spread, limit).reshape(-1)
        lists, flows, arrived, rights = {}, {}, [], (peer[0], peer[1])

        def forward(c, step, x):
            flows[c, step] = lax.ppermute(x, "z", [(step - 1, step), (zs - step, zs - step - 1)])

        def deliver(group):
            terms = [x for c in group for x in (lists[c][-1], *(flows[c, step] for step in range(1, zs)))]
            ready = pick(plane, slots, len(group), flat_spread, my_live, terms)
            arrived.append(lax.all_to_all(ready, ("y", "row"), 0, 0, tiled=True))

        for _, kind, c, step in events:
            if kind == "prepare":
                rights = (prepare(meta, (same[0, 0], peer[0], same[0, 1], peer[1])),)
            elif kind == "product":
                pieces = [same[key] for key in chunks[c]]
                lists[c] = products(dims, (*sizes, entries), meta, pairs, flat_index, pieces, rights)
                forward(c, 1, lists[c][0])
            elif kind == "step":
                own = lists[c][step - 1]
                passed = flows[c, step - 1][: own.shape[0]] + own
                forward(c, step, passed)
            elif kind == "early":
                deliver(groups[c])

        deliver(groups[-1])
        plan = []
        for d in range(plane):
            chip = d % rows_n // 2 * ys + d // rows_n
            for g, group in enumerate(groups):
                for at, c in enumerate(group):
                    for slot, (u, half) in enumerate(chunks[c]):
                        row = (chip ^ u) * 2 * h + half * h + d % 2 * (h // 2)
                        plan.append((d, g, at, slot, row, chip * 2 * h))
        return place(tuple(plan), arrived)[None]

    mean = [-(-tiles * (zs - step) // zs) for step in range(1, zs)]
    whole = tuple(min(tiles, (zs - step) * entries) for step in range(1, zs))
    sizes = [tuple(min(m + extra, w) for m, w, extra in zip(mean, whole, (low, *[low + 1] * zs))) for low in (1, 3)]
    which = 0
    for choice in sizes:
        fits = functools.reduce(jnp.logical_and, [need <= size for need, size in zip(needed, choice)])
        which += 1 - fits.astype(jnp.int32)
    sizes.append(whole)
    branches = [functools.partial(run, size) for size in sizes]
    return lax.switch(which, branches, s, index, spread, my_tile, my_live)


def solution(mesh):
    rows_n, cols_n = mesh.shape["row"], mesh.shape["col"]
    ys = 2 if cols_n % 2 == 0 else 1
    fine = Mesh(mesh.devices.reshape(rows_n, cols_n // ys, ys), ("row", "z", "y"))
    return jax.shard_map(
        body,
        mesh=fine,
        in_specs=(P("row", ("z", "y")), P()),
        out_specs=P("row", ("z", "y"), None, None),
        check_vma=False,
    )
```
